128 devices in a mesh: row: 8 (over y, core), col: 16 (over z, x).
Axes of the slice: x: 4, y: 4, z: 4, core: 2. Of those that a mesh axis runs over, the one named last changes fastest.
Arguments:
- strong_amp: float32 [2048, 128, 128], P(('row', 'col')), may hold values from -3 to 3
- strong_rhs: float32 [2048, 128, 128], P(('row', 'col')), may hold values from -6 to 6
- strong_left: bfloat16 [2048, 128, 128], P(('row', 'col')), may hold values from -0.5 to 0.5
- strong_right: bfloat16 [2048, 128, 128], P(('row', 'col')), may hold values from -0.5 to 0.5
- strong_energy: float32 [2048, 128], P(('row', 'col')), may hold values from 1 to 4
- strong_intersection: bfloat16 [2048, 16, 128, 128], P(('row', 'col')), may hold values from -0.375 to 0.375
- strong_nb: int32 [2048, 16], P(('row', 'col')), may hold values from 0 to 63
- strong_live: int32 [2048], P(('row', 'col')), may hold values from 1 to 16
- col_send: int32 [2048, 2], P(('row', 'col')), may hold values from 0 to 15
- row_send: int32 [1024, 2], P(('row', 'col')), may hold values from 0 to 15
- weak_amp: float32 [4096, 64, 64], P(('row', 'col')), may hold values from -3 to 3
- weak_rhs: float32 [4096, 64, 64], P(('row', 'col')), may hold values from -6 to 6
- weak_blocks: bfloat16 [4096, 64, 128], P(('row', 'col')), may hold values from -0.75 to 0.75
- weak_energy: float32 [4096, 64], P(('row', 'col')), may hold values from 1 to 4
- weak_intersection: bfloat16 [4096, 16, 64, 128], P(('row', 'col')), may hold values from -0.375 to 0.375
- weak_nb: int32 [4096, 16], P(('row', 'col')), may hold values from 0 to 63
Outputs:
- strong_next: float32 [2048, 128, 128], P(('row', 'col'))
- weak_next: float32 [4096, 64, 64], P(('row', 'col'))
The draws below stay inside these ranges and needn't reach their ends.
Inputs may be any that keep to these rules, and one draw needn't show every extreme that they name: `col_send`: entries name local strong pairs of the sending device. `row_send`: entries name local strong pairs of the sending device. `strong_nb`: entries index the reading device's pool. `weak_nb`: entries index the reading device's pool. The first strong_live neighbours of a pair are in use.
All inputs are finite; a program needn't handle non-finite values.
Results may differ from the reference program's by a relative error of at most 0.0024.
Values may be sent and summed in bfloat16 or wider, within the bound.
A program may use at most 128 MiB of HBM per device.

```python
import jax
import jax.numpy as jnp
from jax import lax

P_SIZE = 128
Q = 64
NB = 16
CAP = 2
UPDATES = 2
SP_DEV = 16
WP_DEV = 32
NS = 2048
NW = 4096
POOL = 64
N_ROW = 8
N_COL = 16
DEVICES = 128


def with_ends(entries, own_key, least, high):
    longest = entries.shape.index(max(entries.shape))
    spots = []
    for shift in (0, 1):
        where = [jax.random.randint(jax.random.fold_in(own_key, axis), (), 0, length) for axis, length in enumerate(entries.shape)]
        where[longest] = (where[longest] + shift) % entries.shape[longest]
        spots.append(tuple(where))
    return entries.at[spots[0]].set(least).at[spots[1]].set(high)


def block_levels(own_key, shape, split, least, largest):
    gain, own = 1.0, jax.random.fold_in(own_key, 6)
    for axis_at, shards_of in split:
        steps = jnp.exp(jax.random.uniform(jax.random.fold_in(own, axis_at), (shards_of,), jnp.float32, least / len(split), largest / len(split)))
        gain = gain * jnp.repeat(steps, shape[axis_at] // shards_of).reshape([-1 if axis == axis_at else 1 for axis in range(len(shape))])
    return gain


def normal_values(own_key, dims, deviation, most, shards=(), kind=jnp.bfloat16):
    entries = jax.random.normal(own_key, dims, jnp.float32) * deviation
    if len(shards) > 0:
        entries = block_levels(own_key, dims, shards, -0.22, 0.18) * entries
    return jnp.clip(entries, min=-most, max=most).astype(kind)


def setup_inputs(seed: int = 0) -> dict:
    arg_keys = jax.random.split(jax.random.key(seed), 17)
    return {
        "strong_amp": normal_values(arg_keys[0], (NS, P_SIZE, P_SIZE), 0.5, 3.0, ((0, 128),), jnp.float32),
        "strong_rhs": normal_values(arg_keys[1], (NS, P_SIZE, P_SIZE), 1.0, 6.0, ((0, 128),), jnp.float32),
        "strong_left": normal_values(arg_keys[2], (NS, P_SIZE, P_SIZE), P_SIZE ** -0.5, 0.5, ((0, 128),)),
        "strong_right": normal_values(arg_keys[3], (NS, P_SIZE, P_SIZE), P_SIZE ** -0.5, 0.5, ((0, 128),)),
        "strong_energy": jnp.clip(1.0 + 3.0 * jax.random.uniform(arg_keys[4], (NS, P_SIZE), jnp.float32) ** block_levels(arg_keys[4], (NS, P_SIZE), ((0, 128),), -0.2, 0.2), 1.0, 4.0),
        "strong_intersection": normal_values(arg_keys[5], (NS, NB, P_SIZE, P_SIZE), (2 * P_SIZE) ** -0.5, 0.375, ((0, 128),)),
        "strong_nb": with_ends(jax.random.randint(arg_keys[6], (NS, NB), 0, POOL), jax.random.fold_in(arg_keys[6], 1), 0, POOL - 1).astype(jnp.int32),
        "strong_live": with_ends(jax.random.randint(arg_keys[7], (NS,), 1, NB + 1), jax.random.fold_in(arg_keys[7], 1), 1, NB).astype(jnp.int32),
        "col_send": with_ends(jax.random.randint(arg_keys[8], (DEVICES * N_COL, CAP), 0, SP_DEV), jax.random.fold_in(arg_keys[8], 1), 0, SP_DEV - 1).astype(jnp.int32),
        "row_send": with_ends(jax.random.randint(arg_keys[9], (DEVICES * N_ROW, CAP), 0, SP_DEV), jax.random.fold_in(arg_keys[9], 1), 0, SP_DEV - 1).astype(jnp.int32),
        "weak_amp": normal_values(arg_keys[10], (NW, Q, Q), 0.5, 3.0, ((0, 128),), jnp.float32),
        "weak_rhs": normal_values(arg_keys[11], (NW, Q, Q), 1.0, 6.0, ((0, 128),), jnp.float32),
        "weak_blocks": normal_values(arg_keys[12], (NW, Q, 2 * Q), Q ** -0.5, 0.75, ((0, 128),)),
        "weak_energy": jnp.clip(1.0 + 3.0 * jax.random.uniform(arg_keys[13], (NW, Q), jnp.float32) ** block_levels(arg_keys[13], (NW, Q), ((0, 128),), -0.2, 0.2), 1.0, 4.0),
        "weak_intersection": normal_values(arg_keys[14], (NW, NB, Q, P_SIZE), (2 * P_SIZE) ** -0.5, 0.375, ((0, 128),)),
        "weak_nb": with_ends(jax.random.randint(arg_keys[15], (NW, NB), 0, POOL), jax.random.fold_in(arg_keys[15], 1), 0, POOL - 1).astype(jnp.int32),
    }


def gather_pool(tiles, col_lists, row_lists, row_index, col_index):
    col_ids = jnp.arange(N_COL, dtype=jnp.int32)[:, None]
    row_ids = jnp.arange(N_ROW, dtype=jnp.int32)[:, None]
    own_row = tiles[row_index]
    col_pool = own_row[col_ids, col_lists[row_index, :, col_index, :]]
    own_col = tiles[:, col_index]
    row_pool = own_col[row_ids, row_lists[:, col_index, row_index, :]]
    local = own_row[col_index]
    return jnp.concatenate([local, col_pool.reshape(-1, P_SIZE, P_SIZE), row_pool.reshape(-1, P_SIZE, P_SIZE)], axis=0)


def sandwich(intersection, gathered, live_mask):
    half_way = jnp.einsum('snab,snbc->snac', intersection.astype(jnp.float32), gathered.astype(jnp.float32))
    half_way = half_way.astype(jnp.bfloat16).astype(jnp.float32) * live_mask
    return jnp.einsum('snac,sndc->sad', half_way, intersection.astype(jnp.float32))


def advance(amplitude, rhs, left, right, energy, coupling):
    tiles_now = amplitude.astype(jnp.bfloat16).astype(jnp.float32)
    inter = jnp.einsum('sab,sbc->sac', left.astype(jnp.float32), tiles_now)
    inter = inter + jnp.einsum('sab,sbc->sac', tiles_now, right.astype(jnp.float32))
    residual = rhs + inter + coupling
    return amplitude - residual / (energy[:, :, None] + energy[:, None, :])


def reference(strong_amp, strong_rhs, strong_left, strong_right, strong_energy, strong_intersection, strong_nb, strong_live, col_send, row_send, weak_amp, weak_rhs, weak_blocks, weak_energy, weak_intersection, weak_nb):
    count = N_ROW * N_COL
    col_lists = col_send.reshape(N_ROW, N_COL, N_COL, CAP)
    row_lists = row_send.reshape(N_ROW, N_COL, N_ROW, CAP)
    fixed_items = (
        strong_rhs.reshape(count, SP_DEV, P_SIZE, P_SIZE),
        strong_left.reshape(count, SP_DEV, P_SIZE, P_SIZE),
        strong_right.reshape(count, SP_DEV, P_SIZE, P_SIZE),
        strong_energy.reshape(count, SP_DEV, P_SIZE),
        strong_intersection.reshape(count, SP_DEV, NB, P_SIZE, P_SIZE),
        strong_nb.reshape(count, SP_DEV, NB),
        strong_live.reshape(count, SP_DEV),
        weak_rhs.reshape(count, WP_DEV, Q, Q),
        weak_blocks.reshape(count, WP_DEV, Q, 2 * Q),
        weak_energy.reshape(count, WP_DEV, Q),
        weak_intersection.reshape(count, WP_DEV, NB, Q, P_SIZE),
        weak_nb.reshape(count, WP_DEV, NB),
    )
    indices = jnp.arange(count, dtype=jnp.int32)
    for update_step in range(UPDATES):
        tiles = strong_amp.astype(jnp.bfloat16).reshape(N_ROW, N_COL, SP_DEV, P_SIZE, P_SIZE)

        def per_device(items):
            index, amplitude, weak_now, rhs, left, right, energy, intersection, neighbours, live, wrhs, wblocks, wenergy, woverlap, wneighbours = items
            row_index = index // N_COL
            col_index = index % N_COL
            tile_pool = gather_pool(tiles, col_lists, row_lists, row_index, col_index)
            live_mask = (jnp.arange(NB, dtype=jnp.int32)[None, :] < live[:, None]).astype(jnp.float32)[:, :, None, None]
            strong = advance(amplitude, rhs, left, right, energy, sandwich(intersection, tile_pool[neighbours], live_mask))
            ones = jnp.ones((WP_DEV, NB, 1, 1), jnp.float32)
            weak_coupling = sandwich(woverlap, tile_pool[wneighbours], ones)
            weak = advance(weak_now, wrhs, wblocks[:, :, :Q], wblocks[:, :, Q:], wenergy, weak_coupling)
            return strong, weak

        strong_blocks, weak_blocks_new = lax.map(per_device, (indices, strong_amp.reshape(count, SP_DEV, P_SIZE, P_SIZE), weak_amp.reshape(count, WP_DEV, Q, Q)) + fixed_items)
        strong_amp = strong_blocks.reshape(count * SP_DEV, P_SIZE, P_SIZE)
        weak_amp = weak_blocks_new.reshape(count * WP_DEV, Q, Q)
    return strong_amp, weak_amp
```

```python
import jax
import jax.numpy as jnp
from jax import lax
from jax.experimental import pallas as pl
from jax.experimental.pallas import tpu as pltpu
from jax.sharding import PartitionSpec as P

F32, BF16 = jnp.float32, jnp.bfloat16
MESH = pl.DeviceIdType.MESH
COLS, ROWS, CAP = 16, 8, 2
SIDE, DEPTH, CORES = 4, 4, 2
SP, WP, NB, WIDE, SLIM = 16, 32, 16, 128, 64
POOL, BLANK = 64, 64
ROW_AT = SP + COLS * CAP

COL_STEPS = sorted(
    ((dz, dx) for dz in range(SIDE) for dx in range(SIDE) if dz or dx),
    key=lambda s: -(min(s[0], SIDE - s[0]) + min(s[1], SIDE - s[1])),
)
ROW_STEPS = sorted(
    ((dy, dk) for dy in range(DEPTH) for dk in range(CORES) if dy or dk),
    key=lambda s: -min(s[0], DEPTH - s[0]),
)


def nn(a, b):
    return lax.dot_general(a, b, (((1,), (0,)), ((), ())), preferred_element_type=F32)


def nt(a, b):
    return lax.dot_general(a, b, (((1,), (1,)), ((), ())), preferred_element_type=F32)


def coupling(overlap, pair, pool, tile_of):
    mids = [nn(overlap[pair, n], pool[tile_of(n)]).astype(BF16) for n in range(NB)]
    total = None
    for n in range(0, NB, 2):
        term = nt(
            jnp.concatenate([mids[n], mids[n + 1]], 1),
            jnp.concatenate([overlap[pair, n], overlap[pair, n + 1]], 1),
        )
        total = term if total is None else total + term
    return total


def looped(count, unroll, body):
    def step(i, carry):
        for u in range(unroll):
            body(i * unroll + u)
        return carry

    lax.fori_loop(0, count // unroll, step, 0)


def kernel(
    s_nb, s_live, c_send, r_send, w_nb,
    s_amp_h, s_rhs_h, s_left_h, s_right_h, s_en, s_over_h,
    w_amp_h, w_rhs_h, w_blk_h, w_en, w_over_h,
    s_out_h, w_out_h,
    s_over, w_over, s_amp, s_next, s_rhs, s_left, s_right,
    w_amp, w_next, w_rhs, w_blk, s_inv, w_inv, s_base, w_base,
    pool_a, pool_b, col_a, col_b, row_a, row_b,
    load_sem, out_sem, col_ss, col_rs, row_ss, row_rs,
):
    r, c = lax.axis_index("row"), lax.axis_index("col")
    z, x = c // SIDE, lax.rem(c, SIDE)
    y, k = r // CORES, lax.rem(r, CORES)

    def col_of(step):
        return lax.rem(z + step[0], SIDE) * SIDE + lax.rem(x + step[1], SIDE)

    def row_of(step):
        return lax.rem(y + step[0], DEPTH) * CORES + lax.rem(k + step[1], CORES)

    loads = [
        pltpu.make_async_copy(source, place, load_sem.at[i])
        for i, (source, place) in enumerate(
            (
                (s_amp_h, s_amp), (s_left_h, s_left), (s_right_h, s_right), (s_rhs_h, s_rhs),
                (w_amp_h, w_amp), (w_blk_h, w_blk), (w_rhs_h, w_rhs), (s_over_h, s_over), (w_over_h, w_over),
            )
        )
    ]
    for load in loads:
        load.start()

    barrier = pltpu.get_barrier_semaphore()
    for step in COL_STEPS:
        pl.semaphore_signal(barrier, inc=1, device_id=(r, col_of(step)), device_id_type=MESH)
    for step in ROW_STEPS:
        pl.semaphore_signal(barrier, inc=1, device_id=(row_of(step), c), device_id_type=MESH)

    def exchange(amp, pool, col_buf, row_buf, update, ready):
        base_col, base_row = update * COLS, update * ROWS

        def tile(wanted):
            return amp[wanted].astype(BF16)

        copies = []
        legs = []
        for i in range(max(len(COL_STEPS), len(ROW_STEPS))):
            if i < len(COL_STEPS):
                to = col_of(COL_STEPS[i])
                legs.append((to, c_send, col_buf.at[i], SP + CAP * c, (r, to), col_ss.at[base_col + i], col_rs.at[base_col + i]))
            if i < len(ROW_STEPS):
                to = row_of(ROW_STEPS[i])
                legs.append((to, r_send, row_buf.at[i], ROW_AT + CAP * r, (to, c), row_ss.at[base_row + i], row_rs.at[base_row + i]))
        for to, wanted, buf, at, device, ss, rs in legs:
            for slot in range(CAP):
                buf[slot] = tile(wanted[to, slot])
            copies.append(
                pltpu.make_async_remote_copy(buf, pool.at[pl.ds(at, CAP)], ss, rs, device_id=device, device_id_type=MESH)
            )
            if ready is None:
                copies[-1].start()
        if ready is not None:
            ready()
            for copy in copies:
                copy.start()
        for slot in range(CAP):
            pool[SP + CAP * c + slot] = tile(c_send[c, slot])
            pool[ROW_AT + CAP * r + slot] = tile(r_send[r, slot])

        def own(p):
            pool[p] = tile(p)

        looped(SP, 4, own)
        pool[BLANK] = jnp.zeros((WIDE, WIDE), BF16)
        return copies

    def strong_base(amp):
        def body(p):
            now = amp[p].astype(BF16)
            s_base[p] = s_rhs[p] + nn(s_left[p], now) + nn(now, s_right[p])

        looped(SP, 2, body)

    def weak_base(amp):
        def body(w):
            now = amp[w].astype(BF16)
            w_base[w] = w_rhs[w] + nn(w_blk[w, :, :SLIM], now) + nn(now, w_blk[w, :, SLIM:])

        looped(WP, 4, body)

    def strong_update(amp, new, pool):
        def body(p):
            total = coupling(s_over, p, pool, lambda n: jnp.where(n < s_live[p], s_nb[p, n], BLANK))
            new[p] = amp[p] - (s_base[p] + total) * s_inv[p]

        looped(SP, 2, body)

    def weak_update(amp, new, pool):
        def body(w):
            total = coupling(w_over, w, pool, lambda n: w_nb[w, n])
            new[w] = amp[w] - (w_base[w] + total) * w_inv[w]

        looped(WP, 4, body)

    loads[0].wait()
    copies = exchange(s_amp, pool_a, col_a, row_a, 0, lambda: pl.semaphore_wait(barrier, len(COL_STEPS) + len(ROW_STEPS)))

    def strong_inverse(p):
        across = jnp.broadcast_to(s_en[pl.ds(p, 1), :], (WIDE, WIDE))
        s_inv[p] = 1.0 / (across + across.T)

    def weak_inverse(w):
        across = jnp.broadcast_to(w_en[pl.ds(w, 1), :], (SLIM, SLIM))
        w_inv[w] = 1.0 / (across + across.T)

    looped(SP, 2, strong_inverse)
    looped(WP, 2, weak_inverse)
    for load in loads[1:]:
        load.wait()
    strong_base(s_amp)
    weak_base(w_amp)
    for copy in copies:
        copy.wait()

    strong_update(s_amp, s_next, pool_a)
    copies = exchange(s_next, pool_b, col_b, row_b, 1, None)
    strong_base(s_next)
    weak_update(w_amp, w_next, pool_a)
    weak_base(w_next)
    for copy in copies:
        copy.wait()

    weak_update(w_next, w_amp, pool_b)
    weak_out = pltpu.make_async_copy(w_amp, w_out_h, out_sem.at[0])
    weak_out.start()
    strong_update(s_next, s_amp, pool_b)
    strong_out = pltpu.make_async_copy(s_amp, s_out_h, out_sem.at[1])
    strong_out.start()
    weak_out.wait()
    strong_out.wait()


def on_device(
    strong_amp, strong_rhs, strong_left, strong_right, strong_energy, strong_intersection, strong_nb, strong_live,
    col_send, row_send, weak_amp, weak_rhs, weak_blocks, weak_energy, weak_intersection, weak_nb,
):
    smem, vmem = pl.BlockSpec(memory_space=pltpu.SMEM), pl.BlockSpec(memory_space=pltpu.VMEM)
    hbm = pl.BlockSpec(memory_space=pltpu.HBM)
    strong, weak = (SP, WIDE, WIDE), (WP, SLIM, SLIM)
    return pl.pallas_call(
        kernel,
        out_shape=(jax.ShapeDtypeStruct(strong, F32), jax.ShapeDtypeStruct(weak, F32)),
        in_specs=[smem] * 5 + [hbm] * 4 + [vmem, hbm] + [hbm] * 3 + [vmem, hbm],
        out_specs=(hbm, hbm),
        scratch_shapes=[
            pltpu.VMEM((SP, NB, WIDE, WIDE), BF16),
            pltpu.VMEM((WP, NB, SLIM, WIDE), BF16),
            pltpu.VMEM(strong, F32),
            pltpu.VMEM(strong, F32),
            pltpu.VMEM(strong, F32),
            pltpu.VMEM(strong, BF16),
            pltpu.VMEM(strong, BF16),
            pltpu.VMEM(weak, F32),
            pltpu.VMEM(weak, F32),
            pltpu.VMEM(weak, F32),
            pltpu.VMEM((WP, SLIM, WIDE), BF16),
            pltpu.VMEM(strong, F32),
            pltpu.VMEM(weak, F32),
            pltpu.VMEM(strong, F32),
            pltpu.VMEM(weak, F32),
            pltpu.VMEM((POOL + 1, WIDE, WIDE), BF16),
            pltpu.VMEM((POOL + 1, WIDE, WIDE), BF16),
            pltpu.VMEM((len(COL_STEPS), CAP, WIDE, WIDE), BF16),
            pltpu.VMEM((len(COL_STEPS), CAP, WIDE, WIDE), BF16),
            pltpu.VMEM((len(ROW_STEPS), CAP, WIDE, WIDE), BF16),
            pltpu.VMEM((len(ROW_STEPS), CAP, WIDE, WIDE), BF16),
            pltpu.SemaphoreType.DMA((9,)),
            pltpu.SemaphoreType.DMA((2,)),
            pltpu.SemaphoreType.DMA((2 * COLS,)),
            pltpu.SemaphoreType.DMA((2 * COLS,)),
            pltpu.SemaphoreType.DMA((2 * ROWS,)),
            pltpu.SemaphoreType.DMA((2 * ROWS,)),
        ],
        compiler_params=pltpu.CompilerParams(
            collective_id=0, has_side_effects=True, vmem_limit_bytes=56 * 2**20
        ),
        name="amplitude_updates",
    )(
        strong_nb, strong_live, col_send, row_send, weak_nb,
        strong_amp, strong_rhs, strong_left, strong_right, strong_energy, strong_intersection,
        weak_amp, weak_rhs, weak_blocks, weak_energy, weak_intersection,
    )


def solution(mesh):
    pairs = ("row", "col")
    three, two = P(pairs, None, None), P(pairs, None)
    four = P(pairs, None, None, None)
    in_specs = (
        three, three, three, three, two, four, two, P(pairs),
        two, two, three, three, three, two, four, two,
    )
    return jax.shard_map(
        on_device, mesh=mesh, in_specs=in_specs, out_specs=(three, three), check_vma=False
    )
```

```python
import jax
import jax.numpy as jnp
from jax import lax
from jax.experimental import pallas as pl
from jax.experimental.pallas import tpu as pltpu
from jax.sharding import PartitionSpec as P

F32, BF16 = jnp.float32, jnp.bfloat16
MESH = pl.DeviceIdType.MESH
COLS, ROWS, CAP = 16, 8, 2
SIDE, DEPTH, CORES = 4, 4, 2
SP, WP, NB, WIDE, SLIM = 16, 32, 16, 128, 64
POOL, BLANK = 64, 64
ROW_AT = SP + COLS * CAP

COL_STEPS = sorted(
    ((dz, dx) for dz in range(SIDE) for dx in range(SIDE) if dz or dx),
    key=lambda s: -(min(s[0], SIDE - s[0]) + min(s[1], SIDE - s[1])),
)
ROW_STEPS = sorted(
    ((dy, dk) for dy in range(DEPTH) for dk in range(CORES) if dy or dk),
    key=lambda s: -min(s[0], DEPTH - s[0]),
)


def nn(a, b):
    return lax.dot_general(a, b, (((1,), (0,)), ((), ())), preferred_element_type=F32)


def nt(a, b):
    return lax.dot_general(a, b, (((1,), (1,)), ((), ())), preferred_element_type=F32)


def coupling(overlap, pair, pool, tile_of):
    mids = [nn(overlap[pair, n], pool[tile_of(n)]).astype(BF16) for n in range(NB)]
    total = None
    for n in range(0, NB, 2):
        term = nt(
            jnp.concatenate([mids[n], mids[n + 1]], 1),
            jnp.concatenate([overlap[pair, n], overlap[pair, n + 1]], 1),
        )
        total = term if total is None else total + term
    return total


def looped(count, unroll, body):
    def step(i, carry):
        for u in range(unroll):
            body(i * unroll + u)
        return carry

    lax.fori_loop(0, count // unroll, step, 0)


def first_update(
    s_nb, s_live, c_send, r_send, w_nb,
    s_amp_h, s_rhs_h, s_left_h, s_right_h, s_en, s_over_h,
    w_amp_h, w_rhs_h, w_blk_h, w_en, w_over_h,
    s_over, w_over, pool_b, s_pre, w_pre, s_inv, w_inv,
    s_amp, s_next, s_rhs, s_left, s_right, w_amp, w_next, w_rhs, w_blk, s_base, w_base,
    pool_a, col_a, col_b, row_a, row_b,
    load_sem, col_ss, col_rs, row_ss, row_rs,
):
    r, c = lax.axis_index("row"), lax.axis_index("col")
    z, x = c // SIDE, lax.rem(c, SIDE)
    y, k = r // CORES, lax.rem(r, CORES)

    def col_of(step):
        return lax.rem(z + step[0], SIDE) * SIDE + lax.rem(x + step[1], SIDE)

    def row_of(step):
        return lax.rem(y + step[0], DEPTH) * CORES + lax.rem(k + step[1], CORES)

    loads = [
        pltpu.make_async_copy(source, place, load_sem.at[i])
        for i, (source, place) in enumerate(
            (
                (s_amp_h, s_amp), (s_left_h, s_left), (s_right_h, s_right), (s_rhs_h, s_rhs),
                (w_amp_h, w_amp), (w_blk_h, w_blk), (w_rhs_h, w_rhs), (s_over_h, s_over), (w_over_h, w_over),
            )
        )
    ]
    for load in loads:
        load.start()

    barrier = pltpu.get_barrier_semaphore()
    for step in COL_STEPS:
        pl.semaphore_signal(barrier, inc=1, device_id=(r, col_of(step)), device_id_type=MESH)
    for step in ROW_STEPS:
        pl.semaphore_signal(barrier, inc=1, device_id=(row_of(step), c), device_id_type=MESH)

    def exchange(amp, pool, col_buf, row_buf, update, ready):
        base_col, base_row = update * COLS, update * ROWS

        def tile(wanted):
            return amp[wanted].astype(BF16)

        copies = []
        legs = []
        for i in range(max(len(COL_STEPS), len(ROW_STEPS))):
            if i < len(COL_STEPS):
                to = col_of(COL_STEPS[i])
                legs.append((to, c_send, col_buf.at[i], SP + CAP * c, (r, to), col_ss.at[base_col + i], col_rs.at[base_col + i]))
            if i < len(ROW_STEPS):
                to = row_of(ROW_STEPS[i])
                legs.append((to, r_send, row_buf.at[i], ROW_AT + CAP * r, (to, c), row_ss.at[base_row + i], row_rs.at[base_row + i]))
        for to, wanted, buf, at, device, ss, rs in legs:
            for slot in range(CAP):
                buf[slot] = tile(wanted[slot, to])
            copies.append(
                pltpu.make_async_remote_copy(buf, pool.at[pl.ds(at, CAP)], ss, rs, device_id=device, device_id_type=MESH)
            )
            if ready is None:
                copies[-1].start()
        if ready is not None:
            ready()
            for copy in copies:
                copy.start()
        for slot in range(CAP):
            pool[SP + CAP * c + slot] = tile(c_send[slot, c])
            pool[ROW_AT + CAP * r + slot] = tile(r_send[slot, r])

        def own(p):
            pool[p] = tile(p)

        looped(SP, 4, own)
        pool[BLANK] = jnp.zeros((WIDE, WIDE), BF16)
        return copies

    def strong_base(amp, out):
        def body(p):
            now = amp[p].astype(BF16)
            rest = s_rhs[p] + nn(s_left[p], now) + nn(now, s_right[p])
            out[p] = amp[p] - rest * s_inv[p]

        looped(SP, 4, body)

    def weak_base(amp, out):
        def body(w):
            now = amp[w].astype(BF16)
            rest = w_rhs[w] + nn(w_blk[w, :, :SLIM], now) + nn(now, w_blk[w, :, SLIM:])
            out[w] = amp[w] - rest * w_inv[w]

        looped(WP, 8, body)

    def strong_update(new, pool):
        def body(p):
            total = coupling(s_over, p, pool, lambda n: jnp.where(n < s_live[p], s_nb[p, n], BLANK))
            new[p] = s_base[p] - total * s_inv[p]

        looped(SP, 4, body)

    def weak_update(new, pool):
        def body(w):
            total = coupling(w_over, w, pool, lambda n: w_nb[n, w])
            new[w] = w_base[w] - total * w_inv[w]

        looped(WP, 8, body)

    loads[0].wait()
    copies = exchange(s_amp, pool_a, col_a, row_a, 0, lambda: pl.semaphore_wait(barrier, len(COL_STEPS) + len(ROW_STEPS)))

    def strong_inverse(p):
        across = jnp.broadcast_to(s_en[pl.ds(p, 1), :], (WIDE, WIDE))
        s_inv[p] = 1.0 / (across + across.T)

    def weak_inverse(w):
        across = jnp.broadcast_to(w_en[pl.ds(w, 1), :], (SLIM, SLIM))
        w_inv[w] = 1.0 / (across + across.T)

    looped(SP, 2, strong_inverse)
    looped(WP, 2, weak_inverse)
    for load in loads[1:]:
        load.wait()
    strong_base(s_amp, s_base)
    weak_base(w_amp, w_base)
    for copy in copies:
        copy.wait()

    strong_update(s_next, pool_a)
    copies = exchange(s_next, pool_b, col_b, row_b, 1, None)
    strong_base(s_next, s_pre)
    weak_update(w_next, pool_a)
    weak_base(w_next, w_pre)
    for copy in copies:
        copy.wait()


UNIT, UNITS, WEAK_STEP = 4, 8, 8


def second_update(
    s_nb, s_live, w_nb, s_over, w_over, pool, s_pre, w_pre, s_inv, w_inv,
    s_out, w_out, s_sum, s_new, w_new, s_sem, w_sem,
):
    def parts(p):
        return lax.div(s_live[p] + (UNIT - 1), UNIT)

    total = parts(0)
    for p in range(1, SP):
        total = total + parts(p)

    def strong_units(state):
        p, j = state
        for _ in range(UNITS):
            real = p < SP
            at = jnp.minimum(p, SP - 1)
            live = jnp.where(real, s_live[at], 0)
            mids = [
                nn(s_over[at, j + t], pool[jnp.where(j + t < live, s_nb[at, j + t], BLANK)]).astype(BF16)
                for t in range(UNIT)
            ]
            term = None
            for t in range(0, UNIT, 2):
                more = nt(
                    jnp.concatenate([mids[t], mids[t + 1]], 1),
                    jnp.concatenate([s_over[at, j + t], s_over[at, j + t + 1]], 1),
                )
                term = more if term is None else term + more
            s_sum[p] = jnp.where(j == 0, 0.0, s_sum[p]) + term
            last = j + UNIT >= live
            p = jnp.where(last & real, p + 1, p)
            j = jnp.where(last, 0, j + UNIT)
        return p, j

    def weak_copy(i):
        rows = pl.ds(i * WEAK_STEP, WEAK_STEP)
        return pltpu.make_async_copy(w_new.at[rows], w_out.at[rows], w_sem.at[i])

    def both(i, state):
        for u in range(WEAK_STEP):
            w = i * WEAK_STEP + u
            w_new[w] = w_pre[w] - coupling(w_over, w, pool, lambda n: w_nb[n, w]) * w_inv[w]
        state = strong_units(state)
        weak_copy(i).start()
        return state

    steps = WP // WEAK_STEP
    state = lax.fori_loop(0, steps, both, (jnp.int32(0), jnp.int32(0)))
    rounds = lax.div(total + (UNITS - 1), UNITS)
    lax.fori_loop(steps, rounds, lambda _, state: strong_units(state), state)

    quarter = SP // 4
    copies = []
    for q in range(4):
        for p in range(q * quarter, (q + 1) * quarter):
            s_new[p] = s_pre[p] - s_sum[p] * s_inv[p]
        rows = pl.ds(q * quarter, quarter)
        copies.append(pltpu.make_async_copy(s_new.at[rows], s_out.at[rows], s_sem.at[q]))
        copies[-1].start()
    for i in range(steps):
        weak_copy(i).wait()
    for copy in copies:
        copy.wait()


def on_device(
    strong_amp, strong_rhs, strong_left, strong_right, strong_energy, strong_intersection, strong_nb, strong_live,
    col_send, row_send, weak_amp, weak_rhs, weak_blocks, weak_energy, weak_intersection, weak_nb,
):
    smem, vmem = pl.BlockSpec(memory_space=pltpu.SMEM), pl.BlockSpec(memory_space=pltpu.VMEM)
    hbm = pl.BlockSpec(memory_space=pltpu.HBM)
    strong, weak = (SP, WIDE, WIDE), (WP, SLIM, SLIM)
    tiles = (POOL + 1, WIDE, WIDE)

    def stay(x):
        return pltpu.with_memory_space_constraint(x, pltpu.HBM)

    kept = pl.pallas_call(
        first_update,
        out_shape=(
            pltpu.VMEM((SP, NB, WIDE, WIDE), BF16),
            pltpu.VMEM((WP, NB, SLIM, WIDE), BF16),
            pltpu.VMEM(tiles, BF16),
            pltpu.VMEM(strong, F32),
            pltpu.VMEM(weak, F32),
            pltpu.VMEM(strong, F32),
            pltpu.VMEM(weak, F32),
        ),
        in_specs=[smem] * 5 + [hbm] * 4 + [vmem, hbm] + [hbm] * 3 + [vmem, hbm],
        out_specs=(vmem,) * 7,
        scratch_shapes=[
            pltpu.VMEM(strong, F32),
            pltpu.VMEM(strong, F32),
            pltpu.VMEM(strong, F32),
            pltpu.VMEM(strong, BF16),
            pltpu.VMEM(strong, BF16),
            pltpu.VMEM(weak, F32),
            pltpu.VMEM(weak, F32),
            pltpu.VMEM(weak, F32),
            pltpu.VMEM((WP, SLIM, WIDE), BF16),
            pltpu.VMEM(strong, F32),
            pltpu.VMEM(weak, F32),
            pltpu.VMEM(tiles, BF16),
            pltpu.VMEM((len(COL_STEPS), CAP, WIDE, WIDE), BF16),
            pltpu.VMEM((len(COL_STEPS), CAP, WIDE, WIDE), BF16),
            pltpu.VMEM((len(ROW_STEPS), CAP, WIDE, WIDE), BF16),
            pltpu.VMEM((len(ROW_STEPS), CAP, WIDE, WIDE), BF16),
            pltpu.SemaphoreType.DMA((9,)),
            pltpu.SemaphoreType.DMA((2 * COLS,)),
            pltpu.SemaphoreType.DMA((2 * COLS,)),
            pltpu.SemaphoreType.DMA((2 * ROWS,)),
            pltpu.SemaphoreType.DMA((2 * ROWS,)),
        ],
        compiler_params=pltpu.CompilerParams(
            collective_id=0, has_side_effects=True, vmem_limit_bytes=32 * 2**20
        ),
        name="first_update",
    )(
        strong_nb, strong_live, col_send.T, row_send.T, weak_nb.T,
        stay(strong_amp), stay(strong_rhs), stay(strong_left), stay(strong_right), strong_energy,
        stay(strong_intersection), stay(weak_amp), stay(weak_rhs), stay(weak_blocks), weak_energy,
        stay(weak_intersection),
    )
    return pl.pallas_call(
        second_update,
        out_shape=(jax.ShapeDtypeStruct(strong, F32), jax.ShapeDtypeStruct(weak, F32)),
        in_specs=[smem] * 3 + [vmem] * 7,
        out_specs=(hbm, hbm),
        scratch_shapes=[
            pltpu.VMEM((SP + 1, WIDE, WIDE), F32),
            pltpu.VMEM(strong, F32),
            pltpu.VMEM(weak, F32),
            pltpu.SemaphoreType.DMA((4,)),
            pltpu.SemaphoreType.DMA((WP // WEAK_STEP,)),
        ],
        compiler_params=pltpu.CompilerParams(vmem_limit_bytes=24 * 2**20),
        name="second_update",
    )(strong_nb, strong_live, weak_nb.T, *kept)


def solution(mesh):
    pairs = ("row", "col")
    three, two = P(pairs, None, None), P(pairs, None)
    four = P(pairs, None, None, None)
    in_specs = (
        three, three, three, three, two, four, two, P(pairs),
        two, two, three, three, three, two, four, two,
    )
    return jax.shard_map(
        on_device, mesh=mesh, in_specs=in_specs, out_specs=(three, three), check_vma=False
    )
```

```python
import jax
import jax.numpy as jnp
from jax import lax
from jax.experimental import pallas as pl
from jax.experimental.pallas import tpu as pltpu
from jax.sharding import PartitionSpec as P

F32, BF16 = jnp.float32, jnp.bfloat16
MESH = pl.DeviceIdType.MESH
COLS, ROWS, CAP = 16, 8, 2
SIDE, DEPTH, CORES = 4, 4, 2
SP, WP, NB, WIDE, SLIM = 16, 32, 16, 128, 64
POOL, BLANK = 64, 64
ROW_AT = SP + COLS * CAP

COL_STEPS = sorted(
    ((dz, dx) for dz in range(SIDE) for dx in range(SIDE) if dz or dx),
    key=lambda s: -(min(s[0], SIDE - s[0]) + min(s[1], SIDE - s[1])),
)
ROW_STEPS = sorted(
    ((dy, dk) for dy in range(DEPTH) for dk in range(CORES) if dy or dk),
    key=lambda s: -min(s[0], DEPTH - s[0]),
)


def nn(a, b):
    return lax.dot_general(a, b, (((1,), (0,)), ((), ())), preferred_element_type=F32)


def nt(a, b):
    return lax.dot_general(a, b, (((1,), (1,)), ((), ())), preferred_element_type=F32)


def coupling(overlap, pair, pool, tile_of):
    mids = [nn(overlap[pair, n], pool[tile_of(n)]).astype(BF16) for n in range(NB)]
    total = None
    for n in range(0, NB, 2):
        term = nt(
            jnp.concatenate([mids[n], mids[n + 1]], 1),
            jnp.concatenate([overlap[pair, n], overlap[pair, n + 1]], 1),
        )
        total = term if total is None else total + term
    return total


def looped(count, unroll, body):
    def step(i, carry):
        for u in range(unroll):
            body(i * unroll + u)
        return carry

    lax.fori_loop(0, count // unroll, step, 0)


def first_update(
    s_nb, s_live, c_send, r_send, w_nb,
    s_amp_h, s_rhs_h, s_left_h, s_right_h, s_en, s_over_h,
    w_amp_h, w_rhs_h, w_blk_h, w_en, w_over_h,
    s_over, w_over, pool_b, s_pre, w_pre, s_inv, w_inv,
    s_amp, s_next, s_rhs, s_left, s_right, w_amp, w_next, w_rhs, w_blk, s_base, w_base,
    pool_a, col_a, col_b, row_a, row_b,
    load_sem, col_ss, col_rs, row_ss, row_rs,
):
    r, c = lax.axis_index("row"), lax.axis_index("col")
    z, x = c // SIDE, lax.rem(c, SIDE)
    y, k = r // CORES, lax.rem(r, CORES)

    def col_of(step):
        return lax.rem(z + step[0], SIDE) * SIDE + lax.rem(x + step[1], SIDE)

    def row_of(step):
        return lax.rem(y + step[0], DEPTH) * CORES + lax.rem(k + step[1], CORES)

    barrier = pltpu.get_barrier_semaphore()
    for step in COL_STEPS:
        pl.semaphore_signal(barrier, inc=1, device_id=(r, col_of(step)), device_id_type=MESH)
    for step in ROW_STEPS:
        pl.semaphore_signal(barrier, inc=1, device_id=(row_of(step), c), device_id_type=MESH)

    loads = [
        pltpu.make_async_copy(source, place, load_sem.at[i])
        for i, (source, place) in enumerate(
            (
                (s_amp_h, s_amp), (s_left_h, s_left), (s_right_h, s_right), (s_rhs_h, s_rhs),
                (w_amp_h, w_amp), (w_blk_h, w_blk), (w_rhs_h, w_rhs), (s_over_h, s_over), (w_over_h, w_over),
            )
        )
    ]
    for load in loads:
        load.start()

    def exchange(amp, pool, col_buf, row_buf, update, ready):
        base_col, base_row = update * COLS, update * ROWS

        def tile(wanted):
            return amp[wanted].astype(BF16)

        copies = []
        legs = []
        for i in range(max(len(COL_STEPS), len(ROW_STEPS))):
            if i < len(COL_STEPS):
                to = col_of(COL_STEPS[i])
                legs.append((to, c_send, col_buf.at[i], SP + CAP * c, (r, to), col_ss.at[base_col + i], col_rs.at[base_col + i]))
            if i < len(ROW_STEPS):
                to = row_of(ROW_STEPS[i])
                legs.append((to, r_send, row_buf.at[i], ROW_AT + CAP * r, (to, c), row_ss.at[base_row + i], row_rs.at[base_row + i]))
        for to, wanted, buf, at, device, ss, rs in legs:
            for slot in range(CAP):
                buf[slot] = tile(wanted[slot, to])
            copies.append(
                pltpu.make_async_remote_copy(buf, pool.at[pl.ds(at, CAP)], ss, rs, device_id=device, device_id_type=MESH)
            )
            if ready is None:
                copies[-1].start()
        if ready is not None:
            ready()
            for copy in copies:
                copy.start()
        for slot in range(CAP):
            pool[SP + CAP * c + slot] = tile(c_send[slot, c])
            pool[ROW_AT + CAP * r + slot] = tile(r_send[slot, r])

        def own(p):
            pool[p] = tile(p)

        looped(SP, 4, own)
        pool[BLANK] = jnp.zeros((WIDE, WIDE), BF16)
        return copies

    def strong_base(amp, out):
        def body(p):
            now = amp[p].astype(BF16)
            rest = s_rhs[p] + nn(s_left[p], now) + nn(now, s_right[p])
            out[p] = amp[p] - rest * s_inv[p]

        looped(SP, 4, body)

    def weak_base(amp, out):
        def body(w):
            now = amp[w].astype(BF16)
            rest = w_rhs[w] + nn(w_blk[w, :, :SLIM], now) + nn(now, w_blk[w, :, SLIM:])
            out[w] = amp[w] - rest * w_inv[w]

        looped(WP, 8, body)

    def strong_update(new, pool):
        def body(p):
            total = coupling(s_over, p, pool, lambda n: jnp.where(n < s_live[p], s_nb[p, n], BLANK))
            new[p] = s_base[p] - total * s_inv[p]

        looped(SP, 8, body)

    def weak_update(new, pool):
        def body(w):
            total = coupling(w_over, w, pool, lambda n: w_nb[n, w])
            new[w] = w_base[w] - total * w_inv[w]

        looped(WP, 8, body)

    loads[0].wait()
    copies = exchange(s_amp, pool_a, col_a, row_a, 0, lambda: pl.semaphore_wait(barrier, len(COL_STEPS) + len(ROW_STEPS)))

    def strong_inverse(p):
        across = jnp.broadcast_to(s_en[pl.ds(p, 1), :], (WIDE, WIDE))
        s_inv[p] = 1.0 / (across + across.T)

    def weak_inverse(w):
        across = jnp.broadcast_to(w_en[pl.ds(w, 1), :], (SLIM, SLIM))
        w_inv[w] = 1.0 / (across + across.T)

    looped(SP, 2, strong_inverse)
    looped(WP, 2, weak_inverse)
    for load in loads[1:]:
        load.wait()
    strong_base(s_amp, s_base)
    weak_base(w_amp, w_base)
    for copy in copies:
        copy.wait()

    strong_update(s_next, pool_a)
    copies = exchange(s_next, pool_b, col_b, row_b, 1, None)
    strong_base(s_next, s_pre)
    weak_update(w_next, pool_a)
    weak_base(w_next, w_pre)
    for copy in copies:
        copy.wait()


STRONG_STEP, WEAK_STEP = 8, 16


def second_update(
    s_nb, s_live, w_nb, s_over, w_over, pool, s_pre, w_pre, s_inv, w_inv,
    s_out, w_out, s_new, w_new, s_sem, w_sem,
):
    def strong_copy(i):
        rows = pl.ds(i * STRONG_STEP, STRONG_STEP)
        return pltpu.make_async_copy(s_new.at[rows], s_out.at[rows], s_sem.at[i])

    def weak_copy(i):
        rows = pl.ds(i * WEAK_STEP, WEAK_STEP)
        return pltpu.make_async_copy(w_new.at[rows], w_out.at[rows], w_sem.at[i])

    def strong(i, carry):
        for u in range(STRONG_STEP):
            p = i * STRONG_STEP + u
            total = coupling(s_over, p, pool, lambda n: jnp.where(n < s_live[p], s_nb[p, n], BLANK))
            s_new[p] = s_pre[p] - total * s_inv[p]
        strong_copy(i).start()
        return carry

    def weak(i, carry):
        for u in range(WEAK_STEP):
            w = i * WEAK_STEP + u
            w_new[w] = w_pre[w] - coupling(w_over, w, pool, lambda n: w_nb[n, w]) * w_inv[w]
        weak_copy(i).start()
        return carry

    lax.fori_loop(0, SP // STRONG_STEP, strong, 0)
    lax.fori_loop(0, WP // WEAK_STEP, weak, 0)
    for i in range(SP // STRONG_STEP):
        strong_copy(i).wait()
    for i in range(WP // WEAK_STEP):
        weak_copy(i).wait()


def on_device(
    strong_amp, strong_rhs, strong_left, strong_right, strong_energy, strong_intersection, strong_nb, strong_live,
    col_send, row_send, weak_amp, weak_rhs, weak_blocks, weak_energy, weak_intersection, weak_nb,
):
    smem, vmem = pl.BlockSpec(memory_space=pltpu.SMEM), pl.BlockSpec(memory_space=pltpu.VMEM)
    hbm = pl.BlockSpec(memory_space=pltpu.HBM)
    strong, weak = (SP, WIDE, WIDE), (WP, SLIM, SLIM)
    tiles = (POOL + 1, WIDE, WIDE)

    def stay(x):
        return pltpu.with_memory_space_constraint(x, pltpu.HBM)

    kept = pl.pallas_call(
        first_update,
        out_shape=(
            pltpu.VMEM((SP, NB, WIDE, WIDE), BF16),
            pltpu.VMEM((WP, NB, SLIM, WIDE), BF16),
            pltpu.VMEM(tiles, BF16),
            pltpu.VMEM(strong, F32),
            pltpu.VMEM(weak, F32),
            pltpu.VMEM(strong, F32),
            pltpu.VMEM(weak, F32),
        ),
        in_specs=[smem] * 5 + [hbm] * 4 + [vmem, hbm] + [hbm] * 3 + [vmem, hbm],
        out_specs=(vmem,) * 7,
        scratch_shapes=[
            pltpu.VMEM(strong, F32),
            pltpu.VMEM(strong, F32),
            pltpu.VMEM(strong, F32),
            pltpu.VMEM(strong, BF16),
            pltpu.VMEM(strong, BF16),
            pltpu.VMEM(weak, F32),
            pltpu.VMEM(weak, F32),
            pltpu.VMEM(weak, F32),
            pltpu.VMEM((WP, SLIM, WIDE), BF16),
            pltpu.VMEM(strong, F32),
            pltpu.VMEM(weak, F32),
            pltpu.VMEM(tiles, BF16),
            pltpu.VMEM((len(COL_STEPS), CAP, WIDE, WIDE), BF16),
            pltpu.VMEM((len(COL_STEPS), CAP, WIDE, WIDE), BF16),
            pltpu.VMEM((len(ROW_STEPS), CAP, WIDE, WIDE), BF16),
            pltpu.VMEM((len(ROW_STEPS), CAP, WIDE, WIDE), BF16),
            pltpu.SemaphoreType.DMA((9,)),
            pltpu.SemaphoreType.DMA((2 * COLS,)),
            pltpu.SemaphoreType.DMA((2 * COLS,)),
            pltpu.SemaphoreType.DMA((2 * ROWS,)),
            pltpu.SemaphoreType.DMA((2 * ROWS,)),
        ],
        compiler_params=pltpu.CompilerParams(
            collective_id=0, has_side_effects=True, vmem_limit_bytes=32 * 2**20
        ),
        name="first_update",
    )(
        strong_nb, strong_live, col_send.T, row_send.T, weak_nb.T,
        stay(strong_amp), stay(strong_rhs), stay(strong_left), stay(strong_right), strong_energy,
        stay(strong_intersection), stay(weak_amp), stay(weak_rhs), stay(weak_blocks), weak_energy,
        stay(weak_intersection),
    )
    return pl.pallas_call(
        second_update,
        out_shape=(jax.ShapeDtypeStruct(strong, F32), jax.ShapeDtypeStruct(weak, F32)),
        in_specs=[smem] * 3 + [vmem] * 7,
        out_specs=(hbm, hbm),
        scratch_shapes=[
            pltpu.VMEM(strong, F32),
            pltpu.VMEM(weak, F32),
            pltpu.SemaphoreType.DMA((SP // STRONG_STEP,)),
            pltpu.SemaphoreType.DMA((WP // WEAK_STEP,)),
        ],
        compiler_params=pltpu.CompilerParams(vmem_limit_bytes=24 * 2**20),
        name="second_update",
    )(strong_nb, strong_live, weak_nb.T, *kept)


def solution(mesh):
    pairs = ("row", "col")
    three, two = P(pairs, None, None), P(pairs, None)
    four = P(pairs, None, None, None)
    in_specs = (
        three, three, three, three, two, four, two, P(pairs),
        two, two, three, three, three, two, four, two,
    )
    return jax.shard_map(
        on_device, mesh=mesh, in_specs=in_specs, out_specs=(three, three), check_vma=False
    )
```

```python
import jax
import jax.numpy as jnp
from jax import lax
from jax.experimental import pallas as pl
from jax.experimental.pallas import tpu as pltpu
from jax.sharding import PartitionSpec as P

F32, BF16 = jnp.float32, jnp.bfloat16
MESH = pl.DeviceIdType.MESH
COLS, ROWS, CAP = 16, 8, 2
SIDE, DEPTH, CORES = 4, 4, 2
SP, WP, NB, WIDE, SLIM = 16, 32, 16, 128, 64
POOL, BLANK = 64, 64
ROW_AT = SP + COLS * CAP

COL_STEPS = sorted(
    ((dz, dx) for dz in range(SIDE) for dx in range(SIDE) if dz or dx),
    key=lambda s: -(min(s[0], SIDE - s[0]) + min(s[1], SIDE - s[1])),
)
ROW_STEPS = sorted(
    ((dy, dk) for dy in range(DEPTH) for dk in range(CORES) if dy or dk),
    key=lambda s: -min(s[0], DEPTH - s[0]),
)


def nn(a, b):
    return lax.dot_general(a, b, (((1,), (0,)), ((), ())), preferred_element_type=F32)


def nt(a, b):
    return lax.dot_general(a, b, (((1,), (1,)), ((), ())), preferred_element_type=F32)


def coupling(overlap, pair, pool, tile_of):
    mids = [nn(overlap[pair, n], pool[tile_of(n)]).astype(BF16) for n in range(NB)]
    total = None
    for n in range(0, NB, 2):
        term = nt(
            jnp.concatenate([mids[n], mids[n + 1]], 1),
            jnp.concatenate([overlap[pair, n], overlap[pair, n + 1]], 1),
        )
        total = term if total is None else total + term
    return total


def looped(count, unroll, body):
    def step(i, carry):
        for u in range(unroll):
            body(i * unroll + u)
        return carry

    lax.fori_loop(0, count // unroll, step, 0)


def first_update(
    s_nb_h, s_live_h, c_send_h, r_send_h, w_nb_h,
    s_amp_h, s_rhs_h, s_left_h, s_right_h, s_en_h, s_over_h,
    w_amp_h, w_rhs_h, w_blk_h, w_en_h, w_over_h,
    s_over, w_over, pool_b, s_pre, w_pre, s_inv, w_inv, s_list, w_list,
    s_nb, s_live, c_send, r_send, w_nb, s_en, w_en,
    s_amp, s_next, s_rhs, s_left, s_right, w_amp, w_next, w_rhs, w_blk, s_base, w_base,
    pool_a, col_a, col_b, row_a, row_b,
    load_sem, col_ss, col_rs, row_ss, row_rs,
):
    r, c = lax.axis_index("row"), lax.axis_index("col")
    z, x = c // SIDE, lax.rem(c, SIDE)
    y, k = r // CORES, lax.rem(r, CORES)

    def col_of(step):
        return lax.rem(z + step[0], SIDE) * SIDE + lax.rem(x + step[1], SIDE)

    def row_of(step):
        return lax.rem(y + step[0], DEPTH) * CORES + lax.rem(k + step[1], CORES)

    barrier = pltpu.get_barrier_semaphore()
    for step in COL_STEPS:
        pl.semaphore_signal(barrier, inc=1, device_id=(r, col_of(step)), device_id_type=MESH)
    for step in ROW_STEPS:
        pl.semaphore_signal(barrier, inc=1, device_id=(row_of(step), c), device_id_type=MESH)

    loads = [
        pltpu.make_async_copy(source, place, load_sem.at[i])
        for i, (source, place) in enumerate(
            (
                (c_send_h, c_send), (r_send_h, r_send), (s_amp_h, s_amp),
                (s_en_h, s_en), (w_en_h, w_en), (s_nb_h, s_nb), (s_live_h, s_live), (w_nb_h, w_nb),
                (s_left_h, s_left), (s_right_h, s_right), (s_rhs_h, s_rhs), (w_amp_h, w_amp), (w_blk_h, w_blk), (w_rhs_h, w_rhs), (s_over_h, s_over), (w_over_h, w_over),
            )
        )
    ]
    for load in loads:
        load.start()

    def exchange(amp, pool, col_buf, row_buf, update, ready):
        base_col, base_row = update * COLS, update * ROWS

        def tile(wanted):
            return amp[wanted].astype(BF16)

        copies = []
        legs = []
        for i in range(max(len(COL_STEPS), len(ROW_STEPS))):
            if i < len(COL_STEPS):
                to = col_of(COL_STEPS[i])
                legs.append((to, c_send, col_buf.at[i], SP + CAP * c, (r, to), col_ss.at[base_col + i], col_rs.at[base_col + i]))
            if i < len(ROW_STEPS):
                to = row_of(ROW_STEPS[i])
                legs.append((to, r_send, row_buf.at[i], ROW_AT + CAP * r, (to, c), row_ss.at[base_row + i], row_rs.at[base_row + i]))
        for to, wanted, buf, at, device, ss, rs in legs:
            for slot in range(CAP):
                buf[slot] = tile(wanted[slot, to])
            copies.append(
                pltpu.make_async_remote_copy(buf, pool.at[pl.ds(at, CAP)], ss, rs, device_id=device, device_id_type=MESH)
            )
            if ready is None:
                copies[-1].start()
        if ready is not None:
            ready()
            for copy in copies:
                copy.start()
        for slot in range(CAP):
            pool[SP + CAP * c + slot] = tile(c_send[slot, c])
            pool[ROW_AT + CAP * r + slot] = tile(r_send[slot, r])

        def own(p):
            pool[p] = tile(p)

        looped(SP, 4, own)
        pool[BLANK] = jnp.zeros((WIDE, WIDE), BF16)
        return copies

    def strong_base(amp, out):
        def body(p):
            now = amp[p].astype(BF16)
            rest = s_rhs[p] + nn(s_left[p], now) + nn(now, s_right[p])
            out[p] = amp[p] - rest * s_inv[p]

        looped(SP, 4, body)

    def weak_base(amp, out):
        def body(w):
            now = amp[w].astype(BF16)
            rest = w_rhs[w] + nn(w_blk[w, :, :SLIM], now) + nn(now, w_blk[w, :, SLIM:])
            out[w] = amp[w] - rest * w_inv[w]

        looped(WP, 8, body)

    def strong_update(new, pool):
        def body(p):
            total = coupling(s_over, p, pool, lambda n: s_list[p, n])
            new[p] = s_base[p] - total * s_inv[p]

        looped(SP, 8, body)

    def weak_update(new, pool):
        def body(w):
            total = coupling(w_over, w, pool, lambda n: w_nb[n, w])
            new[w] = w_base[w] - total * w_inv[w]

        looped(WP, 8, body)

    for load in loads[:3]:
        load.wait()
    copies = exchange(s_amp, pool_a, col_a, row_a, 0, lambda: pl.semaphore_wait(barrier, len(COL_STEPS) + len(ROW_STEPS)))

    for load in loads[3:8]:
        load.wait()

    def strong_list(p):
        for n in range(NB):
            s_list[p, n] = jnp.where(n < s_live[p], s_nb[p, n], BLANK)

    def weak_list(n):
        for w in range(WP):
            w_list[n, w] = w_nb[n, w]

    looped(SP, 1, strong_list)
    looped(NB, 1, weak_list)

    def strong_inverse(p):
        across = jnp.broadcast_to(s_en[pl.ds(p, 1), :], (WIDE, WIDE))
        s_inv[p] = 1.0 / (across + across.T)

    def weak_inverse(w):
        across = jnp.broadcast_to(w_en[pl.ds(w, 1), :], (SLIM, SLIM))
        w_inv[w] = 1.0 / (across + across.T)

    looped(SP, 2, strong_inverse)
    looped(WP, 2, weak_inverse)
    for load in loads[8:]:
        load.wait()
    strong_base(s_amp, s_base)
    weak_base(w_amp, w_base)
    for copy in copies:
        copy.wait()

    strong_update(s_next, pool_a)
    copies = exchange(s_next, pool_b, col_b, row_b, 1, None)
    strong_base(s_next, s_pre)
    weak_update(w_next, pool_a)
    weak_base(w_next, w_pre)
    for copy in copies:
        copy.wait()


STRONG_STEP, WEAK_STEP = 8, 16


def second_update(
    s_over, w_over, pool, s_pre, w_pre, s_inv, w_inv, s_list, w_list,
    s_out, w_out, s_new, w_new, s_sem, w_sem,
):
    def strong_copy(i):
        rows = pl.ds(i * STRONG_STEP, STRONG_STEP)
        return pltpu.make_async_copy(s_new.at[rows], s_out.at[rows], s_sem.at[i])

    def weak_copy(i):
        rows = pl.ds(i * WEAK_STEP, WEAK_STEP)
        return pltpu.make_async_copy(w_new.at[rows], w_out.at[rows], w_sem.at[i])

    def strong(i, carry):
        for u in range(STRONG_STEP):
            p = i * STRONG_STEP + u
            total = coupling(s_over, p, pool, lambda n: s_list[p, n])
            s_new[p] = s_pre[p] - total * s_inv[p]
        strong_copy(i).start()
        return carry

    def weak(i, carry):
        for u in range(WEAK_STEP):
            w = i * WEAK_STEP + u
            w_new[w] = w_pre[w] - coupling(w_over, w, pool, lambda n: w_list[n, w]) * w_inv[w]
        weak_copy(i).start()
        return carry

    lax.fori_loop(0, SP // STRONG_STEP, strong, 0)
    lax.fori_loop(0, WP // WEAK_STEP, weak, 0)
    for i in range(SP // STRONG_STEP):
        strong_copy(i).wait()
    for i in range(WP // WEAK_STEP):
        weak_copy(i).wait()


def on_device(
    strong_amp, strong_rhs, strong_left, strong_right, strong_energy, strong_intersection, strong_nb, strong_live,
    col_send, row_send, weak_amp, weak_rhs, weak_blocks, weak_energy, weak_intersection, weak_nb,
):
    smem, vmem = pl.BlockSpec(memory_space=pltpu.SMEM), pl.BlockSpec(memory_space=pltpu.VMEM)
    hbm = pl.BlockSpec(memory_space=pltpu.HBM)
    strong, weak = (SP, WIDE, WIDE), (WP, SLIM, SLIM)
    tiles = (POOL + 1, WIDE, WIDE)

    def stay(x):
        return pltpu.with_memory_space_constraint(x, pltpu.HBM)

    kept = pl.pallas_call(
        first_update,
        out_shape=(
            pltpu.VMEM((SP, NB, WIDE, WIDE), BF16),
            pltpu.VMEM((WP, NB, SLIM, WIDE), BF16),
            pltpu.VMEM(tiles, BF16),
            pltpu.VMEM(strong, F32),
            pltpu.VMEM(weak, F32),
            pltpu.VMEM(strong, F32),
            pltpu.VMEM(weak, F32),
            pltpu.SMEM((SP, NB), jnp.int32),
            pltpu.SMEM((NB, WP), jnp.int32),
        ),
        in_specs=[hbm] * 16,
        out_specs=(vmem,) * 7 + (smem,) * 2,
        scratch_shapes=[
            pltpu.SMEM((SP, NB), jnp.int32),
            pltpu.SMEM((SP,), jnp.int32),
            pltpu.SMEM((CAP, COLS), jnp.int32),
            pltpu.SMEM((CAP, ROWS), jnp.int32),
            pltpu.SMEM((NB, WP), jnp.int32),
            pltpu.VMEM((SP, WIDE), F32),
            pltpu.VMEM((WP, SLIM), F32),
            pltpu.VMEM(strong, F32),
            pltpu.VMEM(strong, F32),
            pltpu.VMEM(strong, F32),
            pltpu.VMEM(strong, BF16),
            pltpu.VMEM(strong, BF16),
            pltpu.VMEM(weak, F32),
            pltpu.VMEM(weak, F32),
            pltpu.VMEM(weak, F32),
            pltpu.VMEM((WP, SLIM, WIDE), BF16),
            pltpu.VMEM(strong, F32),
            pltpu.VMEM(weak, F32),
            pltpu.VMEM(tiles, BF16),
            pltpu.VMEM((len(COL_STEPS), CAP, WIDE, WIDE), BF16),
            pltpu.VMEM((len(COL_STEPS), CAP, WIDE, WIDE), BF16),
            pltpu.VMEM((len(ROW_STEPS), CAP, WIDE, WIDE), BF16),
            pltpu.VMEM((len(ROW_STEPS), CAP, WIDE, WIDE), BF16),
            pltpu.SemaphoreType.DMA((16,)),
            pltpu.SemaphoreType.DMA((2 * COLS,)),
            pltpu.SemaphoreType.DMA((2 * COLS,)),
            pltpu.SemaphoreType.DMA((2 * ROWS,)),
            pltpu.SemaphoreType.DMA((2 * ROWS,)),
        ],
        compiler_params=pltpu.CompilerParams(
            collective_id=0, has_side_effects=True, vmem_limit_bytes=32 * 2**20
        ),
        name="first_update",
    )(
        *map(stay, (
            strong_nb, strong_live, col_send.T, row_send.T, weak_nb.T,
            strong_amp, strong_rhs, strong_left, strong_right, strong_energy, strong_intersection,
            weak_amp, weak_rhs, weak_blocks, weak_energy, weak_intersection,
        )),
    )
    return pl.pallas_call(
        second_update,
        out_shape=(jax.ShapeDtypeStruct(strong, F32), jax.ShapeDtypeStruct(weak, F32)),
        in_specs=[vmem] * 7 + [smem] * 2,
        out_specs=(hbm, hbm),
        scratch_shapes=[
            pltpu.VMEM(strong, F32),
            pltpu.VMEM(weak, F32),
            pltpu.SemaphoreType.DMA((SP // STRONG_STEP,)),
            pltpu.SemaphoreType.DMA((WP // WEAK_STEP,)),
        ],
        compiler_params=pltpu.CompilerParams(vmem_limit_bytes=24 * 2**20),
        name="second_update",
    )(*kept)


def solution(mesh):
    pairs = ("row", "col")
    three, two = P(pairs, None, None), P(pairs, None)
    four = P(pairs, None, None, None)
    in_specs = (
        three, three, three, three, two, four, two, P(pairs),
        two, two, three, three, three, two, four, two,
    )
    return jax.shard_map(
        on_device, mesh=mesh, in_specs=in_specs, out_specs=(three, three), check_vma=False
    )
```

```python
import jax
import jax.numpy as jnp
from jax import lax
from jax.experimental import pallas as pl
from jax.experimental.pallas import tpu as pltpu
from jax.sharding import PartitionSpec as P

F32, BF16 = jnp.float32, jnp.bfloat16
MESH = pl.DeviceIdType.MESH
COLS, ROWS, CAP = 16, 8, 2
SIDE, DEPTH, CORES = 4, 4, 2
SP, WP, NB, WIDE, SLIM = 16, 32, 16, 128, 64
POOL, BLANK = 64, 64
ROW_AT = SP + COLS * CAP

COL_STEPS = sorted(
    ((dz, dx) for dz in range(SIDE) for dx in range(SIDE) if dz or dx),
    key=lambda s: -(min(s[0], SIDE - s[0]) + min(s[1], SIDE - s[1])),
)
ROW_STEPS = sorted(
    ((dy, dk) for dy in range(DEPTH) for dk in range(CORES) if dy or dk),
    key=lambda s: -min(s[0], DEPTH - s[0]),
)


def nn(a, b):
    return lax.dot_general(a, b, (((1,), (0,)), ((), ())), preferred_element_type=F32)


def nt(a, b):
    return lax.dot_general(a, b, (((1,), (1,)), ((), ())), preferred_element_type=F32)


def coupling(overlap, pair, pool, tile_of):
    mids = [nn(overlap[pair, n], pool[tile_of(n)]).astype(BF16) for n in range(NB)]
    total = None
    for n in range(0, NB, 2):
        term = nt(
            jnp.concatenate([mids[n], mids[n + 1]], 1),
            jnp.concatenate([overlap[pair, n], overlap[pair, n + 1]], 1),
        )
        total = term if total is None else total + term
    return total


def looped(count, unroll, body):
    def step(i, carry):
        for u in range(unroll):
            body(i * unroll + u)
        return carry

    lax.fori_loop(0, count // unroll, step, 0)


def first_update(
    s_nb_h, s_live_h, c_send_h, r_send_h, w_nb_h,
    s_amp_h, s_rhs_h, s_left_h, s_right_h, s_en_h, s_over_h,
    w_amp_h, w_rhs_h, w_blk_h, w_en_h, w_over_h,
    s_over, w_over, pool_b, s_pre, w_pre, s_inv, w_inv, s_list, w_list,
    s_nb, s_live, c_send, r_send, w_nb, s_en, w_en,
    s_amp, s_next, s_rhs, s_left, s_right, w_amp, w_next, w_rhs, w_blk, s_base, w_base,
    pool_a, col_a, col_b, row_a, row_b,
    load_sem, col_ss, col_rs, row_ss, row_rs,
):
    r, c = lax.axis_index("row"), lax.axis_index("col")
    z, x = c // SIDE, lax.rem(c, SIDE)
    y, k = r // CORES, lax.rem(r, CORES)

    def col_of(step):
        return lax.rem(z + step[0], SIDE) * SIDE + lax.rem(x + step[1], SIDE)

    def row_of(step):
        return lax.rem(y + step[0], DEPTH) * CORES + lax.rem(k + step[1], CORES)

    barrier = pltpu.get_barrier_semaphore()
    for step in COL_STEPS:
        pl.semaphore_signal(barrier, inc=1, device_id=(r, col_of(step)), device_id_type=MESH)
    for step in ROW_STEPS:
        pl.semaphore_signal(barrier, inc=1, device_id=(row_of(step), c), device_id_type=MESH)

    loads = [
        pltpu.make_async_copy(source, place, load_sem.at[i])
        for i, (source, place) in enumerate(
            (
                (c_send_h, c_send), (r_send_h, r_send), (s_amp_h, s_amp),
                (s_en_h, s_en), (w_en_h, w_en), (s_nb_h, s_nb), (s_live_h, s_live), (w_nb_h, w_nb),
                (s_left_h, s_left), (s_right_h, s_right), (s_rhs_h, s_rhs), (w_amp_h, w_amp), (w_blk_h, w_blk), (w_rhs_h, w_rhs), (s_over_h, s_over), (w_over_h, w_over),
            )
        )
    ]
    for load in loads:
        load.start()

    def exchange(amp, pool, col_buf, row_buf, update, ready):
        base_col, base_row = update * COLS, update * ROWS

        def tile(wanted):
            return amp[wanted].astype(BF16)

        copies = []
        legs = []
        for i in range(max(len(COL_STEPS), len(ROW_STEPS))):
            if i < len(COL_STEPS):
                to = col_of(COL_STEPS[i])
                legs.append((to, c_send, col_buf.at[i], SP + CAP * c, (r, to), col_ss.at[base_col + i], col_rs.at[base_col + i]))
            if i < len(ROW_STEPS):
                to = row_of(ROW_STEPS[i])
                legs.append((to, r_send, row_buf.at[i], ROW_AT + CAP * r, (to, c), row_ss.at[base_row + i], row_rs.at[base_row + i]))
        for to, wanted, buf, at, device, ss, rs in legs:
            for slot in range(CAP):
                buf[slot] = tile(wanted[slot, to])
            copies.append(
                pltpu.make_async_remote_copy(buf, pool.at[pl.ds(at, CAP)], ss, rs, device_id=device, device_id_type=MESH)
            )
            if ready is None:
                copies[-1].start()
        if ready is not None:
            ready()
            for copy in copies:
                copy.start()
        for slot in range(CAP):
            pool[SP + CAP * c + slot] = tile(c_send[slot, c])
            pool[ROW_AT + CAP * r + slot] = tile(r_send[slot, r])

        def own(p):
            pool[p] = tile(p)

        looped(SP, 4, own)
        pool[BLANK] = jnp.zeros((WIDE, WIDE), BF16)
        return copies

    def strong_base(amp, out):
        def body(p):
            now = amp[p].astype(BF16)
            rest = s_rhs[p] + nn(s_left[p], now) + nn(now, s_right[p])
            out[p] = amp[p] - rest * s_inv[p]

        looped(SP, 4, body)

    def weak_base(amp, out):
        def body(w):
            now = amp[w].astype(BF16)
            rest = w_rhs[w] + nn(w_blk[w, :, :SLIM], now) + nn(now, w_blk[w, :, SLIM:])
            out[w] = amp[w] - rest * w_inv[w]

        looped(WP, 8, body)

    def strong_update(new, pool):
        def body(p):
            total = coupling(s_over, p, pool, lambda n: s_list[p, n])
            new[p] = s_base[p] - total * s_inv[p]

        looped(SP, 8, body)

    def weak_update(new, pool):
        def body(w):
            total = coupling(w_over, w, pool, lambda n: w_nb[n, w])
            new[w] = w_base[w] - total * w_inv[w]

        looped(WP, 8, body)

    for load in loads[:3]:
        load.wait()
    copies = exchange(s_amp, pool_a, col_a, row_a, 0, lambda: pl.semaphore_wait(barrier, len(COL_STEPS) + len(ROW_STEPS)))

    for load in loads[3:8]:
        load.wait()

    def strong_list(p):
        for n in range(NB):
            s_list[p, n] = jnp.where(n < s_live[p], s_nb[p, n], BLANK)

    def weak_list(n):
        for w in range(WP):
            w_list[n, w] = w_nb[n, w]

    looped(SP, 1, strong_list)
    looped(NB, 1, weak_list)

    def strong_inverse(p):
        across = jnp.broadcast_to(s_en[pl.ds(p, 1), :], (WIDE, WIDE))
        s_inv[p] = 1.0 / (across + across.T)

    def weak_inverse(w):
        across = jnp.broadcast_to(w_en[pl.ds(w, 1), :], (SLIM, SLIM))
        w_inv[w] = 1.0 / (across + across.T)

    looped(SP, 2, strong_inverse)
    looped(WP, 2, weak_inverse)
    for load in loads[8:]:
        load.wait()
    strong_base(s_amp, s_base)
    weak_base(w_amp, w_base)
    for copy in copies:
        copy.wait()

    strong_update(s_next, pool_a)
    copies = exchange(s_next, pool_b, col_b, row_b, 1, None)
    strong_base(s_next, s_pre)
    weak_update(w_next, pool_a)
    weak_base(w_next, w_pre)
    for copy in copies:
        copy.wait()


STRONG_STEP, WEAK_STEP = 16, 32


def second_update(
    s_over, w_over, pool, s_pre, w_pre, s_inv, w_inv, s_list, w_list,
    s_out, w_out, s_new, w_new, s_sem, w_sem,
):
    def strong_copy(i):
        rows = pl.ds(i * STRONG_STEP, STRONG_STEP)
        return pltpu.make_async_copy(s_new.at[rows], s_out.at[rows], s_sem.at[i])

    def weak_copy(i):
        rows = pl.ds(i * WEAK_STEP, WEAK_STEP)
        return pltpu.make_async_copy(w_new.at[rows], w_out.at[rows], w_sem.at[i])

    def strong(i, carry):
        for u in range(STRONG_STEP):
            p = i * STRONG_STEP + u
            total = coupling(s_over, p, pool, lambda n: s_list[p, n])
            s_new[p] = s_pre[p] - total * s_inv[p]
        strong_copy(i).start()
        return carry

    def weak(i, carry):
        for u in range(WEAK_STEP):
            w = i * WEAK_STEP + u
            w_new[w] = w_pre[w] - coupling(w_over, w, pool, lambda n: w_list[n, w]) * w_inv[w]
        weak_copy(i).start()
        return carry

    lax.fori_loop(0, SP // STRONG_STEP, strong, 0)
    lax.fori_loop(0, WP // WEAK_STEP, weak, 0)
    for i in range(SP // STRONG_STEP):
        strong_copy(i).wait()
    for i in range(WP // WEAK_STEP):
        weak_copy(i).wait()


def on_device(
    strong_amp, strong_rhs, strong_left, strong_right, strong_energy, strong_intersection, strong_nb, strong_live,
    col_send, row_send, weak_amp, weak_rhs, weak_blocks, weak_energy, weak_intersection, weak_nb,
):
    smem, vmem = pl.BlockSpec(memory_space=pltpu.SMEM), pl.BlockSpec(memory_space=pltpu.VMEM)
    hbm = pl.BlockSpec(memory_space=pltpu.HBM)
    strong, weak = (SP, WIDE, WIDE), (WP, SLIM, SLIM)
    tiles = (POOL + 1, WIDE, WIDE)

    def stay(x):
        return pltpu.with_memory_space_constraint(x, pltpu.HBM)

    kept = pl.pallas_call(
        first_update,
        out_shape=(
            pltpu.VMEM((SP, NB, WIDE, WIDE), BF16),
            pltpu.VMEM((WP, NB, SLIM, WIDE), BF16),
            pltpu.VMEM(tiles, BF16),
            pltpu.VMEM(strong, F32),
            pltpu.VMEM(weak, F32),
            pltpu.VMEM(strong, F32),
            pltpu.VMEM(weak, F32),
            pltpu.SMEM((SP, NB), jnp.int32),
            pltpu.SMEM((NB, WP), jnp.int32),
        ),
        in_specs=[hbm] * 16,
        out_specs=(vmem,) * 7 + (smem,) * 2,
        scratch_shapes=[
            pltpu.SMEM((SP, NB), jnp.int32),
            pltpu.SMEM((SP,), jnp.int32),
            pltpu.SMEM((CAP, COLS), jnp.int32),
            pltpu.SMEM((CAP, ROWS), jnp.int32),
            pltpu.SMEM((NB, WP), jnp.int32),
            pltpu.VMEM((SP, WIDE), F32),
            pltpu.VMEM((WP, SLIM), F32),
            pltpu.VMEM(strong, F32),
            pltpu.VMEM(strong, F32),
            pltpu.VMEM(strong, F32),
            pltpu.VMEM(strong, BF16),
            pltpu.VMEM(strong, BF16),
            pltpu.VMEM(weak, F32),
            pltpu.VMEM(weak, F32),
            pltpu.VMEM(weak, F32),
            pltpu.VMEM((WP, SLIM, WIDE), BF16),
            pltpu.VMEM(strong, F32),
            pltpu.VMEM(weak, F32),
            pltpu.VMEM(tiles, BF16),
            pltpu.VMEM((len(COL_STEPS), CAP, WIDE, WIDE), BF16),
            pltpu.VMEM((len(COL_STEPS), CAP, WIDE, WIDE), BF16),
            pltpu.VMEM((len(ROW_STEPS), CAP, WIDE, WIDE), BF16),
            pltpu.VMEM((len(ROW_STEPS), CAP, WIDE, WIDE), BF16),
            pltpu.SemaphoreType.DMA((16,)),
            pltpu.SemaphoreType.DMA((2 * COLS,)),
            pltpu.SemaphoreType.DMA((2 * COLS,)),
            pltpu.SemaphoreType.DMA((2 * ROWS,)),
            pltpu.SemaphoreType.DMA((2 * ROWS,)),
        ],
        compiler_params=pltpu.CompilerParams(
            collective_id=0, has_side_effects=True, vmem_limit_bytes=32 * 2**20
        ),
        name="first_update",
    )(
        *map(stay, (
            strong_nb, strong_live, col_send.T, row_send.T, weak_nb.T,
            strong_amp, strong_rhs, strong_left, strong_right, strong_energy, strong_intersection,
            weak_amp, weak_rhs, weak_blocks, weak_energy, weak_intersection,
        )),
    )
    return pl.pallas_call(
        second_update,
        out_shape=(jax.ShapeDtypeStruct(strong, F32), jax.ShapeDtypeStruct(weak, F32)),
        in_specs=[vmem] * 7 + [smem] * 2,
        out_specs=(hbm, hbm),
        scratch_shapes=[
            pltpu.VMEM(strong, F32),
            pltpu.VMEM(weak, F32),
            pltpu.SemaphoreType.DMA((SP // STRONG_STEP,)),
            pltpu.SemaphoreType.DMA((WP // WEAK_STEP,)),
        ],
        compiler_params=pltpu.CompilerParams(vmem_limit_bytes=24 * 2**20),
        name="second_update",
    )(*kept)


def solution(mesh):
    pairs = ("row", "col")
    three, two = P(pairs, None, None), P(pairs, None)
    four = P(pairs, None, None, None)
    in_specs = (
        three, three, three, three, two, four, two, P(pairs),
        two, two, three, three, three, two, four, two,
    )
    return jax.shard_map(
        on_device, mesh=mesh, in_specs=in_specs, out_specs=(three, three), check_vma=False
    )
```
